32 devices in a mesh: section: 8 (over y, x, core), tp: 4 (over z).
Axes of the slice: x: 2, y: 2, z: 4, core: 2. Of those that a mesh axis runs over, the one named last changes fastest.
Arguments:
- param: float32 [512, 3584], P('section', 'tp'), may hold values from -4 to 4
- moment_one: float32 [512, 3584], P('section', 'tp'), may hold values from -2 to 2
- moment_two: float32 [512, 3584], P('section', 'tp'), may hold values from 0.001 to 1
- proj_grad: float32 [512, 3584], P('section', 'tp'), may hold values from -6 to 6
- embed_grad: bfloat16 [4096, 3584], P('section', 'tp'), may hold values from -6 to 6
- token_ids: int32 [4096], P('section'), may hold values from 0 to 511, as said below
- next_ids: int32 [4096], P('section'), may hold values from 0 to 511, as said below
Outputs:
- new_param: float32 [512, 3584], P('section', 'tp')
- new_moment_one: float32 [512, 3584], P('section', 'tp')
- new_moment_two: float32 [512, 3584], P('section', 'tp')
- next_rows: bfloat16 [4096, 3584], P('section')
The draws below stay inside these ranges and needn't reach their ends.
Inputs may be any that keep to these rules, and one draw needn't show every extreme that they name: `token_ids`: in each section index's block of 512 tokens at most 128 ids fall into any one owner's run of 64 table rows (id // 64); in every draw some owner receives exactly 128 from every block. `next_ids`: the same bound of 128 a block and an owner holds, and is reached, as for token_ids.
All inputs are finite; a program needn't handle non-finite values.
Results may differ from the reference program's by a relative error of at most 0.001.
Values may be sent and summed in bfloat16 or wider, within the bound.
A program may use at most 64 MiB of HBM per device.

```python
import math
import jax
import jax.numpy as jnp

D = 3584
ROWS_OWN = 64
TOK_DEV = 512
STEP = 1000
VOCAB = 512
TOKENS = 4096
CAP = 128


def owner_ids(key, salt):
    key = jax.random.fold_in(key, salt)
    blocks = TOKENS // TOK_DEV
    owners = VOCAB // ROWS_OWN
    slots = owners * CAP
    key_common, key_own, key_score, key_rows, key_order = jax.random.split(key, 5)
    common = jax.random.randint(key_common, (), 0, owners)
    single = jax.random.randint(key_own, (blocks,), 0, owners - 1)
    single = single + (single >= common).astype(jnp.int32)
    scores = jax.random.randint(key_score, (blocks, slots), 0, 2 ** 16) * slots + jnp.arange(slots)[None, :]
    slot_owner = jnp.arange(slots) // CAP
    forced = (slot_owner[None, :] == common) | (slot_owner[None, :] == single[:, None])
    scores = jnp.where(forced, scores - 2 ** 28, scores)
    picked = jnp.argsort(scores, axis=1, stable=True)[:, :TOK_DEV]
    owner = picked // CAP
    mixing = jax.random.randint(key_order, (blocks, TOK_DEV), 0, 2 ** 16) * TOK_DEV + jnp.arange(TOK_DEV)[None, :]
    order = jnp.argsort(mixing, axis=1, stable=True)
    owner = jnp.take_along_axis(owner, order, axis=1)
    within = jax.random.randint(key_rows, (blocks, TOK_DEV), 0, ROWS_OWN)
    return (owner * ROWS_OWN + within).reshape(-1).astype(jnp.int32)


def draw_token_ids(key, part):
    return owner_ids(key, 11)


def draw_next_ids(key, part):
    return owner_ids(key, 23)


def steps_of(own_key, extent, pieces, smallest, largest):
    def one(position, parts):
        draws = jax.random.uniform(jax.random.fold_in(jax.random.fold_in(own_key, 6), position), (parts,), jnp.float32, smallest / len(pieces), largest / len(pieces))
        return jnp.repeat(jnp.exp(draws), extent[position] // parts).reshape((-1,) + (1,) * (len(extent) - position - 1))

    loudness = one(*pieces[0])
    for cut in pieces[1:]:
        loudness = loudness * one(*cut)
    return loudness


def gaussian(key, dims, width, reach, shards=(), held_as=jnp.bfloat16):
    factor_of = steps_of(key, dims, shards, -0.22, 0.18) if shards else 1.0
    result = jax.random.normal(key, dims, jnp.float32) * width * factor_of
    return jnp.minimum(jnp.maximum(result, -reach), reach).astype(held_as)


def setup_inputs(seed: int = 0) -> dict:
    key_list = jax.random.split(jax.random.key(seed), 8)
    return {
        "param": gaussian(key_list[0], (VOCAB, D), 0.5, 4.0, ((0, 8), (1, 4)), jnp.float32),
        "moment_one": gaussian(key_list[1], (VOCAB, D), 0.2, 2.0, ((0, 8), (1, 4)), jnp.float32),
        "moment_two": jnp.clip(jnp.exp(math.log(1.0) - 6.9077552 * jax.random.uniform(key_list[2], (VOCAB, D), jnp.float32) ** steps_of(key_list[2], (VOCAB, D), ((0, 8), (1, 4)), -0.2, 0.2)), 0.001, 1.0),
        "proj_grad": gaussian(key_list[3], (VOCAB, D), 1.0, 6.0, ((0, 8), (1, 4)), jnp.float32),
        "embed_grad": gaussian(key_list[4], (TOKENS, D), 1.0, 6.0, ((0, 8), (1, 4))),
        "token_ids": draw_token_ids(jax.random.fold_in(key_list[7], 71), 0),
        "next_ids": draw_next_ids(jax.random.fold_in(key_list[7], 71), 0),
    }


def reference(param, moment_one, moment_two, proj_grad, embed_grad, token_ids, next_ids):
    embed_sum = jnp.zeros((VOCAB, D), jnp.float32).at[token_ids].add(embed_grad.astype(jnp.float32))
    grad = proj_grad + embed_sum
    new_moment_one = 0.9 * moment_one + 0.1 * grad
    new_moment_two = 0.999 * moment_two + 0.001 * grad * grad
    first_fix = 1.0 - 0.9 ** STEP
    second_fix = 1.0 - 0.999 ** STEP
    new_param = param - 0.01 * (new_moment_one / first_fix) / (jnp.sqrt(new_moment_two / second_fix) + 1e-08)
    table = new_param.astype(jnp.bfloat16)
    next_rows = jnp.take(table, next_ids, axis=0)
    return (new_param, new_moment_one, new_moment_two, next_rows)
```

```python
import functools

import jax
import jax.numpy as jnp
from jax import lax
from jax.experimental import pallas as pl
from jax.experimental.pallas import tpu as pltpu
from jax.sharding import PartitionSpec as P

STEP = 1000
MESH = pl.DeviceIdType.MESH


def adam(param, moment_one, moment_two, grad):
    new_moment_one = 0.9 * moment_one + 0.1 * grad
    new_moment_two = 0.999 * moment_two + 0.001 * grad * grad
    first_fix = 1.0 - 0.9**STEP
    second_fix = 1.0 - 0.999**STEP
    new_param = param - 0.01 * (new_moment_one / first_fix) / (
        jnp.sqrt(new_moment_two / second_fix) + 1e-08
    )
    return new_param, new_moment_one, new_moment_two


def chunks_of(width):
    first = -(-(width // 2) // 128) * 128
    return ((0, first), (first, width - first))


def sync_kernel(
    ranks, ids_in, next_in, rows_in, param_in, one_in, two_in, proj_in,
    new_param_out, new_one_out, new_two_out, out_ref,
    new_param_ref, new_one_ref, new_two_ref, found0, found1, state_s, found_s,
    ids_ref, next_ref, rows_ref, param_ref, one_ref, two_ref, proj_ref, load_s,
    pick, mine0, mine1, theirs0, theirs1, from_core0, from_core1, from_chip0, from_chip1,
    table0, table1,
    core_s, core_r, chip_s, chip_r, z_s, z_r, x_s, x_r, y_s, y_r,
    across_s, across_r, pair_s, pair_r, pz_s, pz_r, px_s, px_r, py_s, py_r,
    pacross_s, pacross_r, ppair_s, ppair_r,
):
    rows, width = param_ref.shape
    quarter = rows // 4
    main = rows
    chunks = chunks_of(width)
    mine, theirs = (mine0, mine1), (theirs0, theirs1)
    from_core, from_chip = (from_core0, from_core1), (from_chip0, from_chip1)
    tables, found = (table0, table1), (found0, found1)
    me = lax.axis_index("section")
    z = lax.axis_index("tp")
    core = lax.rem(me, 2)
    x_bit = lax.rem(lax.div(me, 2), 2)
    y_bit = lax.div(me, 4)
    by_core = me + 1 - 2 * core
    by_x = me + 2 - 4 * x_bit
    by_y = me + 4 - 8 * y_bit
    by_both = by_x + by_y - me
    chips = (by_both, by_x, by_y, me)
    has_low, has_high = z > 0, z < ranks - 1
    loads = [
        pltpu.make_async_copy(src, dst, load_s.at[k])
        for k, (src, dst) in enumerate((
            (ids_in, ids_ref), (rows_in, rows_ref), (next_in, next_ref), (proj_in, proj_ref),
            (param_in, param_ref), (one_in, one_ref), (two_in, two_ref),
        ))
    ]
    for one in loads:
        one.start()

    barrier = pltpu.get_barrier_semaphore()
    for other in (by_core, by_x, by_y, by_both):
        pl.semaphore_signal(barrier, inc=1, device_id=(other, z), device_id_type=MESH)

    @pl.when(has_low)
    def _():
        pl.semaphore_signal(barrier, inc=1, device_id=(me, z - 1), device_id_type=MESH)

    @pl.when(has_high)
    def _():
        pl.semaphore_signal(barrier, inc=1, device_id=(me, z + 1), device_id_type=MESH)

    def picks(owner_core):
        local = lax.broadcasted_iota(jnp.int32, (rows, ids_ref.shape[1]), 0)
        hits = []
        for chip in chips:
            first = (lax.div(chip, 2) * 2 + owner_core) * rows
            hit = local == ids_ref[...] - first
            hits.append(jnp.where(hit, 1.0, 0.0).astype(jnp.bfloat16))
        return jnp.concatenate(hits, axis=0)

    def partial_sums(hits, c):
        begin, size = chunks[c]
        return jnp.dot(
            hits, rows_ref[:, begin : begin + size], preferred_element_type=jnp.float32
        ).reshape(len(chips), rows, size)

    def copy(src, dst, send, recv, section, tp):
        return pltpu.make_async_remote_copy(
            src_ref=src, dst_ref=dst, send_sem=send, recv_sem=recv,
            device_id=(section, tp), device_id_type=MESH,
        )

    to_core = [
        [
            copy(theirs[c].at[k], from_core[c].at[k], core_s.at[c, k], core_r.at[c, k], by_core, z)
            for k in range(4)
        ]
        for c in range(2)
    ]
    to_chip = [
        [
            copy(mine[c].at[k], from_chip[c].at[k], chip_s.at[c, k], chip_r.at[c, k], chips[k], z)
            for k in range(3)
        ]
        for c in range(2)
    ]
    loads[0].wait()
    hits = picks(1 - core)
    loads[1].wait()
    theirs[0][...] = partial_sums(hits, 0)
    pl.semaphore_wait(
        barrier, 4 + has_low.astype(jnp.int32) + has_high.astype(jnp.int32)
    )
    for one in to_core[0]:
        one.start()
    theirs[1][...] = partial_sums(hits, 1)
    for one in to_core[1]:
        one.start()
    hits = picks(core)
    for c in range(2):
        mine[c][...] = partial_sums(hits, c)
        for k in range(3):
            to_core[c][k].wait_recv()
            mine[c][k] = mine[c][k] + from_core[c][k]
            to_chip[c][k].start()
    for one in loads[2:]:
        one.wait()
    index = lax.broadcasted_iota(jnp.int32, (pick.shape[1], pick.shape[0]), 0)
    pick[...] = jnp.where(index == next_ref[...], 1.0, 0.0).T.astype(jnp.bfloat16)

    def update(c):
        begin, size = chunks[c]
        cols = slice(begin, begin + size)
        to_core[c][3].wait_recv()
        total = proj_ref[:, cols] + (mine[c][3] + from_core[c][3])
        for k in (1, 2, 0):
            to_chip[c][k].wait_recv()
            total = total + from_chip[c][k]
        new_param, new_one, new_two = adam(
            param_ref[:, cols], one_ref[:, cols], two_ref[:, cols], total
        )
        tables[c][z, pl.ds(pl.multiple_of(me * rows, rows), rows)] = new_param.astype(jnp.bfloat16)
        new_param_ref[:, cols] = new_param
        new_one_ref[:, cols] = new_one
        new_two_ref[:, cols] = new_two

    def at(c, origin, section, first, size):
        begin = pl.multiple_of(section * rows + first, quarter)
        return tables[c].at[origin, pl.ds(begin, size)]

    def same(ref, send, recv, section, tp):
        return copy(ref, ref, send, recv, section, tp)

    states = [
        pltpu.make_async_copy(src, dst, state_s.at[k])
        for k, (src, dst) in enumerate((
            (new_param_ref, new_param_out), (new_one_ref, new_one_out), (new_two_ref, new_two_out),
        ))
    ]

    def main_z(c, o, up):
        return same(
            at(c, o, me, 0, main), z_s.at[c, up, o], z_r.at[c, o], me, z + 2 * up - 1
        )

    def main_x(c, o):
        return same(at(c, o, me, 0, main), x_s.at[c, o], x_r.at[c, o], by_x, z)

    def main_y(c, o):
        return same(at(c, o, me, 0, main), y_s.at[c, o], y_r.at[c, o], by_y, z)

    def main_across(c, o, from_x):
        first, size = (0, rows // 2) if from_x else (rows // 2, rows // 2)
        source, target = (by_x, by_y) if from_x else (by_y, by_x)
        k = int(from_x)
        return same(
            at(c, o, source, first, size), across_s.at[c, k, o], across_r.at[c, k, o], target, z
        )

    def main_pair(c, o, k, section=None):
        section = chips[k] if section is None else section
        return same(
            at(c, o, section, 0, main), pair_s.at[c, k, o], pair_r.at[c, k, o], by_core, z
        )

    def rest_x(c):
        return same(at(c, z, me, main, quarter), px_s.at[c], px_r.at[c], by_x, z)

    def rest_y(c):
        return same(at(c, z, me, main, quarter), py_s.at[c], py_r.at[c], by_y, z)

    def rest_across(c):
        source, target = (by_y, by_x) if c == 0 else (by_x, by_y)
        return same(at(c, z, source, main, quarter), pacross_s.at[c], pacross_r.at[c], target, z)

    def rest_z(c, o, k, up):
        return same(
            at(c, o, chips[k], main, quarter), pz_s.at[c, k, up, o], pz_r.at[c, k, o],
            me, z + 2 * up - 1,
        )

    def rest_pair(c, o, k, section=None):
        section = chips[k] if section is None else section
        return same(
            at(c, o, section, main, quarter), ppair_s.at[c, k, o], ppair_r.at[c, k, o], by_core, z
        )

    def both_z(make):
        pl.when(has_low)(lambda: make(0).start())
        pl.when(has_high)(lambda: make(1).start())

    def begin_gather(c):
        both_z(lambda up: main_z(c, z, up))
        main_x(c, z).start()
        main_y(c, z).start()
        main_pair(c, z, 3).start()

    def rest_near(c):
        for k in ((2, 1) if c == 0 else (1, 2)):
            (rest_x, rest_y)[k - 1](c).wait_recv()
            if k == (2 if c == 0 else 1):
                rest_across(c).start()
            both_z(lambda up: rest_z(c, z, k, up))
            rest_pair(c, z, k).start()

    def rest_far(c):
        rest_across(c).wait_recv()
        both_z(lambda up: rest_z(c, z, 0, up))
        rest_pair(c, z, 0).start()

    def sides(body, distance):
        if distance >= ranks:
            return
        if distance == 0:
            body(z, 0)
            return
        pl.when(z >= distance)(lambda: body(z - distance, 1))
        pl.when(z + distance < ranks)(lambda: body(z + distance, -1))

    def main_from_z(c, distance):
        def body(o, way):
            ref = at(c, o, me, 0, main)
            same(ref, z_s.at[c, 0, o], z_r.at[c, o], me, z - way).wait_recv()
            if way > 0:
                pl.when(has_high)(lambda: main_z(c, o, 1).start())
            else:
                pl.when(has_low)(lambda: main_z(c, o, 0).start())
            main_x(c, o).start()
            main_y(c, o).start()
            main_pair(c, o, 3).start()

        sides(body, distance)

    def rest_from_z(c, distance):
        def body(o, way):
            for k in (3, 1, 2, 0):
                ref = at(c, o, chips[k], main, quarter)
                same(ref, pz_s.at[c, k, 0, o], pz_r.at[c, k, o], me, z - way).wait_recv()
                if way > 0:
                    pl.when(has_high)(lambda: rest_z(c, o, k, 1).start())
                else:
                    pl.when(has_low)(lambda: rest_z(c, o, k, 0).start())
                rest_pair(c, o, k).start()

        sides(body, distance)

    def main_near(c, distance):
        def body(o, way):
            del way
            main_x(c, o).wait_recv()
            main_across(c, o, True).start()
            main_pair(c, o, 1).start()
            main_y(c, o).wait_recv()
            main_across(c, o, False).start()
            main_pair(c, o, 2).start()

        sides(body, distance)

    def main_far(c, distance):
        def body(o, way):
            del way
            main_across(c, o, True).wait_recv()
            main_across(c, o, False).wait_recv()
            main_pair(c, o, 0).start()

        sides(body, distance)

    origins, count = [0] * ranks, 0
    for distance in range(ranks):
        for way in ((0,) if distance == 0 else (-1, 1)):
            value = z + way * distance
            valid = ((value >= 0) & (value < ranks)).astype(jnp.int32)
            for k in range(ranks):
                same_rank = (count == k) if isinstance(count, int) else (count == k).astype(jnp.int32)
                origins[k] = origins[k] + valid * same_rank * value
            count = count + valid

    def found_copy(c, nearest):
        begin, size = chunks[c]
        start = pl.multiple_of(origins[nearest] * width + begin, 128)
        return pltpu.make_async_copy(
            found[c].at[nearest], out_ref.at[:, pl.ds(start, size)], found_s.at[c, nearest]
        )

    def choose(c, nearest):
        if nearest >= ranks:
            return
        o = origins[nearest]
        for k in range(4):
            other = chips[k] + 1 - 2 * core
            main_pair(c, o, k, other).wait_recv()
        found[c][nearest] = jnp.dot(
            pick[...], tables[c][o], preferred_element_type=jnp.float32
        ).astype(jnp.bfloat16)
        found_copy(c, nearest).start()

    update(0)
    begin_gather(0)
    main_from_z(0, 1)
    update(1)
    begin_gather(1)
    for one in states:
        one.start()
    main_from_z(0, 2)
    main_near(0, 0)
    main_from_z(1, 1)
    main_from_z(0, 3)
    main_near(0, 1)
    main_far(0, 0)
    main_from_z(1, 2)
    main_near(1, 0)
    main_near(0, 2)
    main_far(0, 1)
    main_from_z(1, 3)
    choose(0, 0)
    main_near(1, 1)
    main_far(1, 0)
    main_near(0, 3)
    main_far(0, 2)
    choose(0, 1)
    main_near(1, 2)
    main_far(1, 1)
    choose(1, 0)
    main_far(0, 3)
    choose(0, 2)
    main_near(1, 3)
    main_far(1, 2)
    choose(1, 1)
    choose(0, 3)
    choose(1, 2)
    for late in range(4, ranks):
        for c in range(2):
            main_from_z(c, late)
            main_near(c, late)
            main_far(c, late)
            choose(c, late)
    main_far(1, 3)
    choose(1, 3)

    for one in states:
        one.wait()
    for c in range(2):
        for nearest in range(ranks):
            found_copy(c, nearest).wait()
        for one in to_core[c] + to_chip[c]:
            one.wait_send()
        for o in range(ranks):
            for k in range(4):
                main_pair(c, o, k).wait_send()
            main_x(c, o).wait_send()
            main_y(c, o).wait_send()
            main_across(c, o, True).wait_send()
            main_across(c, o, False).wait_send()

            def down(c=c, o=o):
                main_z(c, o, 0).wait_send()

            def up(c=c, o=o):
                main_z(c, o, 1).wait_send()

            pl.when((o >= z) & has_low)(down)
            pl.when((o <= z) & has_high)(up)


def fused(ranks, param, moment_one, moment_two, proj_grad, embed_grad, token_ids, next_ids):
    rows, width = param.shape
    owners = lax.axis_size("section")
    tokens = token_ids.shape[0]
    table_rows = owners * rows
    dma = pltpu.SemaphoreType.DMA
    own = pltpu.VMEM((rows, width), jnp.float32)
    sizes = [size for _, size in chunks_of(width)]

    def sums(count):
        return [pltpu.VMEM((count, rows, size), jnp.float32) for size in sizes]

    results = pl.pallas_call(
        functools.partial(sync_kernel, ranks),
        out_shape=(own, own, own, pltpu.VMEM((tokens, ranks * width), jnp.bfloat16)),
        in_specs=[pl.BlockSpec(memory_space=pltpu.HBM)] * 7,
        out_specs=(pl.BlockSpec(memory_space=pltpu.VMEM),) * 4,
        scratch_shapes=[
            *[pltpu.VMEM((rows, width), jnp.float32)] * 3,
            *[pltpu.VMEM((ranks, tokens, size), jnp.bfloat16) for size in sizes],
            dma((3,)), dma((2, ranks)),
            pltpu.VMEM((1, tokens), jnp.int32), pltpu.VMEM((1, tokens), jnp.int32),
            pltpu.VMEM((tokens, width), jnp.bfloat16),
            *[pltpu.VMEM((rows, width), jnp.float32)] * 4, dma((7,)),
            pltpu.VMEM((tokens, table_rows), jnp.bfloat16),
            *sums(4), *sums(4), *sums(4), *sums(3),
            *[pltpu.VMEM((ranks, table_rows, size), jnp.bfloat16) for size in sizes],
            dma((2, 4)), dma((2, 4)), dma((2, 3)), dma((2, 3)),
            dma((2, 2, ranks)), dma((2, ranks)),
            dma((2, ranks)), dma((2, ranks)), dma((2, ranks)), dma((2, ranks)),
            dma((2, 2, ranks)), dma((2, 2, ranks)), dma((2, 4, ranks)), dma((2, 4, ranks)),
            dma((2, 4, 2, ranks)), dma((2, 4, ranks)),
            dma((2,)), dma((2,)), dma((2,)), dma((2,)), dma((2,)), dma((2,)),
            dma((2, 4, ranks)), dma((2, 4, ranks)),
        ],
        compiler_params=pltpu.CompilerParams(collective_id=0, has_side_effects=True, vmem_limit_bytes=48 * 2 ** 20),
    )(*(
        pltpu.with_memory_space_constraint(one, pltpu.HBM)
        for one in (
            token_ids.reshape(1, tokens), next_ids.reshape(1, tokens), embed_grad,
            param, moment_one, moment_two, proj_grad,
        )
    ))
    return pl.pallas_call(
        hand_over,
        out_shape=tuple(jax.ShapeDtypeStruct(one.shape, one.dtype) for one in results),
        in_specs=[pl.BlockSpec(memory_space=pltpu.VMEM)] * 4,
        out_specs=(pl.BlockSpec(memory_space=pltpu.HBM),) * 4,
        scratch_shapes=[dma((4,))],
        compiler_params=pltpu.CompilerParams(vmem_limit_bytes=16 * 2 ** 20),
    )(*(pltpu.with_memory_space_constraint(one, pltpu.VMEM) for one in results))


def hand_over(*refs):
    done = refs[8]
    copies = [
        pltpu.make_async_copy(src, dst, done.at[k])
        for k, (src, dst) in enumerate(zip(refs[:4], refs[4:8]))
    ]
    for one in copies[::-1]:
        one.start()
    for one in copies:
        one.wait()


def slot_layout(ids, owners, cap, rows_own):
    owner = ids // rows_own
    hits = (owner[:, None] == jnp.arange(owners)[None, :]).astype(jnp.int32)
    before = jnp.cumsum(hits, axis=0) - hits
    rank = jnp.sum(before * hits, axis=1)
    return (owner * cap + rank, ids - owner * rows_own)


def exchange(param, moment_one, moment_two, proj_grad, embed_grad, token_ids, next_ids):
    rows_own, width = param.shape
    owners = lax.axis_size("section")
    tokens_here = token_ids.shape[0]
    cap = 2 * tokens_here // owners
    slot, local = slot_layout(token_ids, owners, cap, rows_own)
    outgoing = jnp.zeros((owners * cap, width), jnp.bfloat16).at[slot].set(embed_grad)
    targets = jnp.full((owners * cap,), -1, jnp.int32).at[slot].set(local)
    got_rows, got_local = (
        lax.all_to_all(
            outgoing.reshape(owners, cap, width), "section", split_axis=0, concat_axis=0, tiled=True
        ),
        lax.all_to_all(
            targets.reshape(owners, cap), "section", split_axis=0, concat_axis=0, tiled=True
        ),
    )
    select = (jnp.arange(rows_own)[:, None] == got_local.reshape(-1)[None, :]).astype(jnp.bfloat16)
    embed_sum = jnp.dot(
        select, got_rows.reshape(owners * cap, width), preferred_element_type=jnp.float32
    )
    grad = proj_grad + embed_sum
    new_param, new_moment_one, new_moment_two = adam(param, moment_one, moment_two, grad)
    table = new_param.astype(jnp.bfloat16)
    piece = lax.all_gather(table, "section", axis=0, tiled=True)
    inside = (next_ids >= 0) & (next_ids < piece.shape[0])
    found = jnp.take(piece, jnp.clip(next_ids, 0, piece.shape[0] - 1), axis=0)
    mine = jnp.where(inside[:, None], found, jnp.zeros((tokens_here, width), jnp.bfloat16))
    next_rows = lax.all_gather(mine, "tp", axis=1, tiled=True)
    return (new_param, new_moment_one, new_moment_two, next_rows)


def solution(mesh):
    placed = (
        P("section", "tp"),
        P("section", "tp"),
        P("section", "tp"),
        P("section", "tp"),
        P("section", "tp"),
        P("section"),
        P("section"),
    )
    ranks = mesh.shape["tp"]

    def on_device(*args):
        owners = mesh.shape["section"]
        table_rows, tokens = args[0].shape[0] * owners, args[5].shape[0]
        if owners == 2 ** 3 and table_rows <= tokens and args[0].shape[0] % 64 == 0 and args[0].shape[1] % 256 in (0, 128):
            return fused(ranks, *args)
        return exchange(*args)

    return jax.shard_map(
        on_device,
        mesh=mesh,
        in_specs=placed,
        out_specs=(P("section", "tp"), P("section", "tp"), P("section", "tp"), P("section", None)),
        check_vma=False,
    )
```

```python
import functools

import jax
import jax.numpy as jnp
from jax import lax
from jax.experimental import pallas as pl
from jax.experimental.pallas import tpu as pltpu
from jax.sharding import PartitionSpec as P

STEP = 1000
MESH = pl.DeviceIdType.MESH


def adam(param, moment_one, moment_two, grad):
    new_moment_one = 0.9 * moment_one + 0.1 * grad
    new_moment_two = 0.999 * moment_two + 0.001 * grad * grad
    first_fix = 1.0 - 0.9**STEP
    second_fix = 1.0 - 0.999**STEP
    new_param = param - 0.01 * (new_moment_one / first_fix) / (
        jnp.sqrt(new_moment_two / second_fix) + 1e-08
    )
    return new_param, new_moment_one, new_moment_two


STEPS = 32000.0


def chunks_of(width):
    first = -(-(width // 2) // 128) * 128
    return ((0, first), (first, width - first))


def sync_kernel(
    ranks, ids_in, next_in, rows_in, param_in, one_in, two_in, proj_in,
    new_param_ref, new_one_ref, new_two_ref, out_ref,
    ids_ref, next_ref, rows0, rows1, state_ref, pick, part0, part1, code0, code1, scale0, scale1,
    got0, got1, got_scale0, got_scale1, table0, table1,
    load_s, core_s, core_r, chip_s, chip_r, z_r, near_r, far_r, rest_r, rest_z_r, pair_r,
    main_s, rest_s, pair_s, z_s,
):
    rows, width = new_param_ref.shape
    rest = rows // 4
    main = rows - rest
    chunks = chunks_of(width)
    tokens_of, part, tables = (rows0, rows1), (part0, part1), (table0, table1)
    code, scale = (code0, code1), (scale0, scale1)
    got, got_scale = (got0, got1), (got_scale0, got_scale1)
    me = lax.axis_index("section")
    z = lax.axis_index("tp")
    core = lax.rem(me, 2)
    x_bit = lax.rem(lax.div(me, 2), 2)
    y_bit = lax.div(me, 4)
    by_core = me + 1 - 2 * core
    by_x = me + 2 - 4 * x_bit
    by_y = me + 4 - 8 * y_bit
    by_both = by_x + by_y - me
    sections = (by_both, by_x, by_y, me)
    chips = tuple(lax.div(one, 2) for one in sections)
    has_low, has_high = z > 0, z < ranks - 1

    def load(src, dst, k):
        return pltpu.make_async_copy(src, dst, load_s.at[k])

    loads = [load(ids_in, ids_ref.at[0], 0)] + [
        load(rows_in.at[:, pl.ds(begin, size)], tokens_of[c].at[0], 1 + c)
        for c, (begin, size) in enumerate(chunks)
    ]
    late = [load(next_in, next_ref, 3)] + [
        load(src, state_ref.at[k], 4) for k, src in enumerate((param_in, one_in, two_in, proj_in))
    ]
    for one in loads + late:
        one.start()

    barrier = pltpu.get_barrier_semaphore()
    for other in (by_core, by_x, by_y, by_both):
        pl.semaphore_signal(barrier, inc=1, device_id=(other, z), device_id_type=MESH)

    @pl.when(has_low)
    def _():
        pl.semaphore_signal(barrier, inc=1, device_id=(me, z - 1), device_id_type=MESH)

    @pl.when(has_high)
    def _():
        pl.semaphore_signal(barrier, inc=1, device_id=(me, z + 1), device_id_type=MESH)

    def copy(src, dst, send, recv, section, tp):
        return pltpu.make_async_remote_copy(
            src_ref=src, dst_ref=dst, send_sem=send, recv_sem=recv,
            device_id=(section, tp), device_id_type=MESH,
        )

    def arrived(ref, semaphore):
        pltpu.make_async_copy(ref, ref, semaphore).wait()

    def hits_of(slot):
        ids = ids_ref[slot]
        local = lax.broadcasted_iota(jnp.int32, (rows, ids.shape[1]), 0)
        return jnp.concatenate(
            [
                jnp.where(local == ids - (2 * chip + core) * rows, 1.0, 0.0).astype(jnp.bfloat16)
                for chip in chips
            ],
            axis=0,
        )

    to_core = [copy(ids_ref.at[0], ids_ref.at[1], core_s.at[2], core_r.at[2], by_core, z)] + [
        copy(one.at[0], one.at[1], core_s.at[c], core_r.at[c], by_core, z)
        for c, one in enumerate(tokens_of)
    ]
    loads[0].wait()
    own_hits = hits_of(0)
    pl.semaphore_wait(
        barrier, 4 + has_low.astype(jnp.int32) + has_high.astype(jnp.int32)
    )
    to_core[0].start()
    for c in range(2):
        loads[1 + c].wait()
        to_core[1 + c].start()

    def own_sums(c):
        part[c][...] = jnp.dot(
            own_hits, tokens_of[c][0], preferred_element_type=jnp.float32
        ).reshape(part[c].shape)

    def send_sums(c):
        to_core[1 + c].wait_recv()
        part[c][...] += jnp.dot(
            other_hits, tokens_of[c][1], preferred_element_type=jnp.float32
        ).reshape(part[c].shape)
        for k in range(3):
            sums = part[c][k]
            top = jnp.maximum(jnp.max(jnp.abs(sums), axis=0, keepdims=True), 1e-30)
            code[c][k] = jnp.round(sums * (STEPS / top)).astype(jnp.int32).astype(jnp.int16)
            scale[c][k] = top * (1.0 / STEPS)
            copy(
                code[c].at[k], got[c].at[k], chip_s.at[c, 0], chip_r.at[c, 0], sections[k], z
            ).start()
            copy(
                scale[c].at[k], got_scale[c].at[k], chip_s.at[c, 1], chip_r.at[c, 1], sections[k], z
            ).start()

    own_sums(0)
    to_core[0].wait_recv()
    other_hits = hits_of(1)
    send_sums(0)
    own_sums(1)
    send_sums(1)
    late[0].wait()
    index = lax.broadcasted_iota(jnp.int32, (pick.shape[1], pick.shape[0]), 0)
    pick[...] = jnp.where(index == next_ref[...], 1.0, 0.0).T.astype(jnp.bfloat16)
    arrived(state_ref, load_s.at[4])

    def at(c, o, chip, first, size):
        return tables[c].at[o, chip, core, pl.ds(first, size)]

    def mains(c, count, chip_count=1):
        return tables[c].at[pl.ds(0, count), pl.ds(0, chip_count), 0, pl.ds(0, main)]

    def rests(c, count, chip_count=4):
        return tables[c].at[pl.ds(0, count), pl.ds(0, chip_count), 0, pl.ds(main, rest)]

    def same(ref, send, recv, section, tp):
        copy(ref, ref, send, recv, section, tp).start()

    def to_pair(c, o, chip, first, size):
        same(at(c, o, chip, first, size), pair_s.at[c], pair_r.at[c, o], by_core, z)

    def to_x(c, o, chip, first, size, send, recv):
        same(at(c, o, chip, first, size), send, recv, by_x, z)

    def to_y(c, o, chip, first, size, send, recv):
        same(at(c, o, chip, first, size), send, recv, by_y, z)

    def along_z(c, kind, ref, recv, way):
        def up():
            same(ref, z_s.at[c, kind, 1], recv, me, z + 1)

        def down():
            same(ref, z_s.at[c, kind, 0], recv, me, z - 1)

        if way >= 0:
            pl.when(has_high)(up)
        if way <= 0:
            pl.when(has_low)(down)

    def spread_main(c, o, way):
        ref = at(c, o, chips[3], 0, main)
        along_z(c, 0, ref, z_r.at[c, o], way)
        to_x(c, o, chips[3], 0, main, main_s.at[c], near_r.at[c, o])
        to_y(c, o, chips[3], 0, main, main_s.at[c], near_r.at[c, o])

    def update(c):
        begin, size = chunks[c]
        cols = slice(begin, begin + size)
        total = state_ref[3, :, cols] + part[c][3]
        arrived(got[c], chip_r.at[c, 0])
        arrived(got_scale[c], chip_r.at[c, 1])
        for k in range(3):
            total = total + got[c][k].astype(jnp.int32).astype(jnp.float32) * got_scale[c][k]
        new_param, new_one, new_two = adam(
            state_ref[0, :, cols], state_ref[1, :, cols], state_ref[2, :, cols], total
        )
        tables[c][z, chips[3], core] = new_param.astype(jnp.bfloat16)
        to_x(c, z, chips[3], main, rest, rest_s.at[c], rest_r.at[c, 0])
        to_y(c, z, chips[3], main, rest, rest_s.at[c], rest_r.at[c, 0])
        spread_main(c, z, 0)
        to_pair(c, z, chips[3], 0, rows)
        new_param_ref[:, cols] = new_param
        new_one_ref[:, cols] = new_one
        new_two_ref[:, cols] = new_two

    def sides(body, distance):
        if distance >= ranks:
            return
        if distance == 0:
            body(z, 0)
            return
        pl.when(z >= distance)(lambda: body(z - distance, 1))
        pl.when(z + distance < ranks)(lambda: body(z + distance, -1))

    def main_from_z(c, distance):
        def body(o, way):
            arrived(at(c, o, chips[3], 0, main), z_r.at[c, o])
            spread_main(c, o, way)
            to_pair(c, o, chips[3], 0, main)

        sides(body, distance)

    def main_near(c, distance):
        def body(o, way):
            del way
            arrived(mains(c, 1, 2), near_r.at[c, o])
            half = main // 32 * 16
            cuts = ((0, half), (half, main - half))
            to_y(c, o, chips[1], *cuts[c], main_s.at[c], far_r.at[c, o])
            to_x(c, o, chips[2], *cuts[1 - c], main_s.at[c], far_r.at[c, o])
            to_pair(c, o, chips[1], 0, main)
            to_pair(c, o, chips[2], 0, main)

        sides(body, distance)

    def main_far(c, distance):
        def body(o, way):
            del way
            arrived(mains(c, 1), far_r.at[c, o])
            to_pair(c, o, chips[0], 0, main)

        sides(body, distance)

    def rest_near(c):
        arrived(rests(c, 1, 2), rest_r.at[c, 0])
        if c == 0:
            to_y(c, z, chips[1], main, rest, rest_s.at[c], rest_r.at[c, 1])
        else:
            to_x(c, z, chips[2], main, rest, rest_s.at[c], rest_r.at[c, 1])
        to_pair(c, z, chips[1], main, rest)
        to_pair(c, z, chips[2], main, rest)

    def all_rest(c, o):
        return tables[c].at[o, pl.ds(0, 4), core, pl.ds(main, rest)]

    def rest_far(c):
        arrived(rests(c, 1, 1), rest_r.at[c, 1])
        along_z(c, 1, all_rest(c, z), rest_z_r.at[c, z], 0)
        to_pair(c, z, chips[0], main, rest)

    def rest_from_z(c, distance):
        def body(o, way):
            ref = all_rest(c, o)
            arrived(ref, rest_z_r.at[c, o])
            along_z(c, 1, ref, rest_z_r.at[c, o], way)
            same(ref, pair_s.at[c], pair_r.at[c, o], by_core, z)

        sides(body, distance)

    origins, count = [0] * ranks, 0
    for distance in range(ranks):
        for way in ((0,) if distance == 0 else (-1, 1)):
            value = z + way * distance
            valid = ((value >= 0) & (value < ranks)).astype(jnp.int32)
            for k in range(ranks):
                same_rank = (count == k) if isinstance(count, int) else (count == k).astype(jnp.int32)
                origins[k] = origins[k] + valid * same_rank * value
            count = count + valid

    def choose(c, nearest):
        if nearest >= ranks:
            return
        o = origins[nearest]
        arrived(tables[c].at[o, pl.ds(0, 4), 0], pair_r.at[c, o])
        begin, size = chunks[c]
        start = pl.multiple_of(o * width + begin, 128)
        out_ref[:, pl.ds(start, size)] = jnp.dot(
            pick[...], tables[c][o].reshape(pick.shape[1], size),
            preferred_element_type=jnp.float32,
        ).astype(jnp.bfloat16)

    update(0)
    rest_near(0)
    update(1)
    main_from_z(0, 1)
    rest_far(0)
    rest_near(1)
    main_from_z(1, 1)
    main_near(1, 0)
    main_from_z(0, 2)
    rest_far(1)
    main_near(0, 0)
    main_from_z(1, 2)
    main_near(0, 1)
    rest_from_z(0, 1)
    main_from_z(0, 3)
    rest_from_z(1, 1)
    main_from_z(1, 3)
    main_far(1, 0)
    main_near(0, 2)
    main_near(1, 1)
    rest_from_z(0, 2)
    main_far(0, 0)
    choose(1, 0)
    main_near(1, 2)
    main_near(0, 3)
    rest_from_z(1, 2)
    main_far(0, 1)
    main_near(1, 3)
    choose(0, 0)
    main_far(0, 2)
    main_far(1, 1)
    main_far(1, 2)
    choose(0, 1)
    main_far(0, 3)
    choose(1, 1)
    rest_from_z(0, 3)
    choose(1, 2)
    main_far(1, 3)
    rest_from_z(1, 3)
    choose(0, 2)
    choose(0, 3)
    choose(1, 3)

    for distance in range(4, ranks):
        for c in range(2):
            main_from_z(c, distance)
            main_near(c, distance)
            main_far(c, distance)
            rest_from_z(c, distance)
            choose(c, distance)

    for one in to_core:
        one.wait_send()
    for c in range(2):
        arrived(code[c], chip_s.at[c, 0])
        arrived(scale[c], chip_s.at[c, 1])
        arrived(mains(c, ranks, 3), main_s.at[c])
        arrived(rests(c, 1, 3), rest_s.at[c])
        arrived(tables[c].at[pl.ds(0, ranks), pl.ds(0, 4), 0], pair_s.at[c])
        for rank in range(ranks):
            def sent(c=c, rank=rank):
                for way, messages in ((1, rank + 1), (0, ranks - rank)):
                    if rank != (ranks - 1) * way:
                        arrived(mains(c, messages), z_s.at[c, 0, way])
                        arrived(rests(c, messages), z_s.at[c, 1, way])

            pl.when(z == rank)(sent)


def fused(ranks, param, moment_one, moment_two, proj_grad, embed_grad, token_ids, next_ids):
    rows, width = param.shape
    owners = lax.axis_size("section")
    tokens = token_ids.shape[0]
    table_rows = owners * rows
    dma = pltpu.SemaphoreType.DMA
    own = pltpu.VMEM((rows, width), jnp.float32)
    sizes = [size for _, size in chunks_of(width)]

    def both(*lead, dtype):
        return [pltpu.VMEM((*lead, size), dtype) for size in sizes]

    results = pl.pallas_call(
        functools.partial(sync_kernel, ranks),
        out_shape=(own, own, own, pltpu.VMEM((tokens, ranks * width), jnp.bfloat16)),
        in_specs=[pl.BlockSpec(memory_space=pltpu.HBM)] * 7,
        out_specs=(pl.BlockSpec(memory_space=pltpu.VMEM),) * 4,
        scratch_shapes=[
            pltpu.VMEM((2, 1, tokens), jnp.int32), pltpu.VMEM((1, tokens), jnp.int32),
            *both(2, tokens, dtype=jnp.bfloat16),
            pltpu.VMEM((4, rows, width), jnp.float32),
            pltpu.VMEM((tokens, table_rows), jnp.bfloat16),
            *both(4, rows, dtype=jnp.float32),
            *both(3, rows, dtype=jnp.int16), *both(3, 1, dtype=jnp.float32),
            *both(3, rows, dtype=jnp.int16), *both(3, 1, dtype=jnp.float32),
            *both(ranks, 4, 2, rows, dtype=jnp.bfloat16),
            dma((5,)), dma((3,)), dma((3,)), dma((2, 2)), dma((2, 2)),
            dma((2, ranks)), dma((2, ranks)), dma((2, ranks)), dma((2, 2)), dma((2, ranks)),
            dma((2, ranks)), dma((2,)), dma((2,)), dma((2,)), dma((2, 2, 2)),
        ],
        compiler_params=pltpu.CompilerParams(
            collective_id=0, has_side_effects=True, vmem_limit_bytes=48 * 2 ** 20
        ),
    )(*(
        pltpu.with_memory_space_constraint(one, pltpu.HBM)
        for one in (
            token_ids.reshape(1, tokens), next_ids.reshape(1, tokens), embed_grad,
            param, moment_one, moment_two, proj_grad,
        )
    ))
    return pl.pallas_call(
        hand_over,
        out_shape=tuple(jax.ShapeDtypeStruct(one.shape, one.dtype) for one in results),
        in_specs=[pl.BlockSpec(memory_space=pltpu.VMEM)] * 4,
        out_specs=(pl.BlockSpec(memory_space=pltpu.HBM),) * 4,
        scratch_shapes=[dma((4,))],
        compiler_params=pltpu.CompilerParams(vmem_limit_bytes=16 * 2 ** 20),
    )(*(pltpu.with_memory_space_constraint(one, pltpu.VMEM) for one in results))


def hand_over(*refs):
    done = refs[8]
    copies = [
        pltpu.make_async_copy(src, dst, done.at[k])
        for k, (src, dst) in enumerate(zip(refs[:4], refs[4:8]))
    ]
    for one in copies[::-1]:
        one.start()
    for one in copies:
        one.wait()


def slot_layout(ids, owners, cap, rows_own):
    owner = ids // rows_own
    hits = (owner[:, None] == jnp.arange(owners)[None, :]).astype(jnp.int32)
    before = jnp.cumsum(hits, axis=0) - hits
    rank = jnp.sum(before * hits, axis=1)
    return (owner * cap + rank, ids - owner * rows_own)


def exchange(param, moment_one, moment_two, proj_grad, embed_grad, token_ids, next_ids):
    rows_own, width = param.shape
    owners = lax.axis_size("section")
    tokens_here = token_ids.shape[0]
    cap = 2 * tokens_here // owners
    slot, local = slot_layout(token_ids, owners, cap, rows_own)
    outgoing = jnp.zeros((owners * cap, width), jnp.bfloat16).at[slot].set(embed_grad)
    targets = jnp.full((owners * cap,), -1, jnp.int32).at[slot].set(local)
    got_rows, got_local = (
        lax.all_to_all(
            outgoing.reshape(owners, cap, width), "section", split_axis=0, concat_axis=0, tiled=True
        ),
        lax.all_to_all(
            targets.reshape(owners, cap), "section", split_axis=0, concat_axis=0, tiled=True
        ),
    )
    select = (jnp.arange(rows_own)[:, None] == got_local.reshape(-1)[None, :]).astype(jnp.bfloat16)
    embed_sum = jnp.dot(
        select, got_rows.reshape(owners * cap, width), preferred_element_type=jnp.float32
    )
    grad = proj_grad + embed_sum
    new_param, new_moment_one, new_moment_two = adam(param, moment_one, moment_two, grad)
    table = new_param.astype(jnp.bfloat16)
    piece = lax.all_gather(table, "section", axis=0, tiled=True)
    inside = (next_ids >= 0) & (next_ids < piece.shape[0])
    found = jnp.take(piece, jnp.clip(next_ids, 0, piece.shape[0] - 1), axis=0)
    mine = jnp.where(inside[:, None], found, jnp.zeros((tokens_here, width), jnp.bfloat16))
    next_rows = lax.all_gather(mine, "tp", axis=1, tiled=True)
    return (new_param, new_moment_one, new_moment_two, next_rows)


def solution(mesh):
    placed = (
        P("section", "tp"),
        P("section", "tp"),
        P("section", "tp"),
        P("section", "tp"),
        P("section", "tp"),
        P("section"),
        P("section"),
    )
    ranks = mesh.shape["tp"]

    def on_device(*args):
        owners = mesh.shape["section"]
        table_rows, tokens = args[0].shape[0] * owners, args[5].shape[0]
        if owners == 2 ** 3 and table_rows <= tokens and args[0].shape[0] % 64 == 0 and args[0].shape[1] % 256 in (0, 128):
            return fused(ranks, *args)
        return exchange(*args)

    return jax.shard_map(
        on_device,
        mesh=mesh,
        in_specs=placed,
        out_specs=(P("section", "tp"), P("section", "tp"), P("section", "tp"), P("section", None)),
        check_vma=False,
    )
```
